32 devices in a mesh: hb: 4 (over y, core), row: 2 (over x), col: 4 (over z).
Axes of the slice: x: 2, y: 2, z: 4, core: 2. Of those that a mesh axis runs over, the one named last changes fastest.
Arguments:
- cell_state: float32 [256, 8, 256, 512], P('hb', None, 'row', 'col'), may hold values from -6 to 6
- normalizer: float32 [256, 8, 256], P('hb', None, 'row'), may hold values from 0.1 to 4
- stabilizer: float32 [256, 8, 16], P('hb', None, 'row'), may hold values from -5 to 120
- queries: float32 [256, 8, 256], P('hb', None, 'row'), may hold values from 0.0125 to 0.1125
- key_vectors: float32 [256, 8, 256], P('hb', None, 'row'), may hold values from -6 to 6
- token_value_vectors: float32 [256, 8, 512], P('hb', None, 'col'), may hold values from -6 to 6
- input_gate: float32 [256, 8], P('hb'), may hold values from -3 to 3
- forget_gate: float32 [256, 8], P('hb'), may hold values from -1 to 5
- output_gate_logits: float32 [256, 8, 512], P('hb', None, 'col'), may hold values from -6 to 6
- norm_gain: float32 [8, 512], P(None, 'col'), may hold values from 0.5 to 1.5
- out_weight: bfloat16 [8, 512, 4096], P('hb', 'col', 'row'), may hold values from -0.09375 to 0.09375
Outputs:
- layer_out: float32 [256, 4096], P('hb', 'row')
- readout: float32 [256, 8, 512], P('hb', None, 'col')
- refreshed_cell: float32 [256, 8, 256, 512], P('hb', None, 'row', 'col')
- new_normal: float32 [256, 8, 256], P('hb', None, 'row')
- new_stab: float32 [256, 8, 16], P('hb', None, 'row')
The draws below stay inside these ranges and needn't reach their ends.
All inputs are finite; a program needn't handle non-finite values.
Results may differ from the reference program's by a relative error of at most 0.0029.
Values may be sent and summed in bfloat16 or wider, within the bound.
A program may use at most 128 MiB of HBM per device.

```python
import math
import jax
import jax.numpy as jnp
from jax import lax

H = 8
DK = 256
DV = 512
D = 4096
RBLK = 16
NBLK = 16
BATCH = 256


def draw_stabilizer(key, part):
    offset_key, spread_key = jax.random.split(jax.random.fold_in(key, 7))
    offset = jax.random.uniform(offset_key, (BATCH, H, 1), jnp.float32, -1.0, 1.0)
    spread_factor = jax.random.uniform(spread_key, (BATCH, H, NBLK), jnp.float32, -1.5, 1.5)
    return offset + spread_factor


def level_of(rng, extent, shards, least, largest):
    factor_of, own = 1.0, jax.random.fold_in(rng, 6)
    for position, shards_of in shards:
        draws = jnp.exp(jax.random.uniform(jax.random.fold_in(own, position), (shards_of,), jnp.float32, least / len(shards), largest / len(shards)))
        factor_of = factor_of * jnp.repeat(draws, extent[position] // shards_of).reshape([-1 if axis == position else 1 for axis in range(len(extent))])
    return factor_of


def centred(rng, shape, scale, limit, cuts=(), kind=jnp.bfloat16):
    level = level_of(rng, shape, cuts, -0.22, 0.18) if cuts else 1.0
    array = jax.random.normal(rng, shape, jnp.float32) * scale * level
    return jnp.minimum(jnp.maximum(array, -limit), limit).astype(kind)


def setup_inputs(seed: int = 0) -> dict:
    streams_of = jax.random.split(jax.random.key(seed), 12)
    cell_state = centred(streams_of[0], (BATCH, H, DK, DV), 1.0, 6.0, ((0, 4), (2, 2), (3, 4)), jnp.float32)
    normalizer = jnp.clip(jnp.exp(math.log(4.0) - 3.6888794 * jax.random.uniform(streams_of[1], (BATCH, H, DK), jnp.float32) ** level_of(streams_of[1], (BATCH, H, DK), ((0, 4), (2, 2)), -0.2, 0.2)), 0.1, 4.0)
    stabilizer = draw_stabilizer(jax.random.fold_in(streams_of[11], 71), 0)
    queries = jnp.clip(0.0125 + 0.099999997 * jax.random.uniform(streams_of[3], (BATCH, H, DK), jnp.float32) ** level_of(streams_of[3], (BATCH, H, DK), ((0, 4), (2, 2)), -0.2, 0.2), 0.0125, 0.1125)
    key_vectors = centred(streams_of[4], (BATCH, H, DK), 1.0, 6.0, ((0, 4), (2, 2)), jnp.float32)
    token_value_vectors = centred(streams_of[5], (BATCH, H, DV), 1.0, 6.0, ((0, 4), (2, 4)), jnp.float32)
    input_gate = jnp.clip(jax.random.uniform(streams_of[6], (BATCH, H), jnp.float32, -3.0, 3.0) * level_of(streams_of[6], (BATCH, H), ((0, 4),), -0.4, 0.0), -3.0, 3.0)
    forget_gate = jnp.clip(-1.0 + 6.0 * jax.random.uniform(streams_of[7], (BATCH, H), jnp.float32) ** level_of(streams_of[7], (BATCH, H), ((0, 4),), -0.2, 0.2), -1.0, 5.0)
    output_gate_logits = centred(streams_of[8], (BATCH, H, DV), 1.0, 6.0, ((0, 4), (2, 4)), jnp.float32)
    norm_gain = jnp.clip(1.0 + 0.1 * jax.random.normal(streams_of[9], (H, DV), jnp.float32), 0.5, 1.5)
    out_weight = centred(streams_of[10], (H, DV, D), (H * DV) ** -0.5, 0.09375, ((0, 4), (1, 4), (2, 2)))
    return {"cell_state": cell_state, "normalizer": normalizer, "stabilizer": stabilizer, "queries": queries, "key_vectors": key_vectors, "token_value_vectors": token_value_vectors, "input_gate": input_gate, "forget_gate": forget_gate, "output_gate_logits": output_gate_logits, "norm_gain": norm_gain, "out_weight": out_weight}


def advance(cell, normal, stabs, query_row, token_key_row, value_row, in_gate, forget_pre):
    carried = jax.nn.log_sigmoid(forget_pre)[:, None] + stabs
    fresh = jnp.maximum(carried, in_gate[:, None])
    keep = jnp.repeat(jnp.exp(carried - fresh), RBLK, axis=1)
    admit = jnp.repeat(jnp.exp(in_gate[:, None] - fresh), RBLK, axis=1)
    scaled = token_key_row * DK ** (-0.5)
    refreshed_cell = keep[:, :, None] * cell + (admit * scaled)[:, :, None] * value_row[:, None, :]
    new_normal = keep * normal + admit * scaled
    top = lax.optimization_barrier(jnp.max(fresh, axis=1))
    weight_matrix = jnp.repeat(jnp.exp(fresh - top[:, None]), RBLK, axis=1) * query_row
    numerator = jnp.einsum('fdo,fd->fo', refreshed_cell, weight_matrix, precision=lax.Precision.HIGHEST)
    denom = lax.optimization_barrier(jnp.sum(new_normal * weight_matrix, axis=1))
    readout = numerator / jnp.maximum(jnp.abs(denom), jnp.exp(-top))[:, None]
    return (refreshed_cell, new_normal, fresh, readout)

def reference(cell_state, normalizer, stabilizer, queries, key_vectors, token_value_vectors, input_gate, forget_gate, output_gate_logits, norm_gain, out_weight):
    refreshed_cell, new_normal, new_stab, readout = lax.map(lambda packed: advance(*packed), (cell_state, normalizer, stabilizer, queries, key_vectors, token_value_vectors, input_gate, forget_gate))
    mean = lax.optimization_barrier(jnp.sum(readout, axis=2)) / DV
    var = lax.optimization_barrier(jnp.sum(readout * readout, axis=2)) / DV - mean * mean
    normed = (readout - mean[:, :, None]) * lax.rsqrt(var + 1e-06)[:, :, None]
    gated = (normed * norm_gain * jax.nn.sigmoid(output_gate_logits)).astype(jnp.bfloat16)
    layer_out = jnp.dot(gated.reshape(gated.shape[0], H * DV), out_weight.reshape(H * DV, D), preferred_element_type=jnp.float32)
    return (layer_out, readout, refreshed_cell, new_normal, new_stab)
```

```python
import functools

import jax
import jax.numpy as jnp
from jax import lax
from jax.experimental import pallas as pl
from jax.experimental.pallas import tpu as pltpu
from jax.sharding import PartitionSpec as P

PAIRS = 32
F32 = jnp.float32
BF16 = jnp.bfloat16


def combined_all(part, axis, combine):
    gathered = jax.tree.map(lambda a: lax.all_gather(a, axis), part)

    def take(source):
        return jax.tree.map(lambda a: lax.dynamic_index_in_dim(a, source, 0, False), gathered)

    return lax.fori_loop(
        1, lax.axis_size(axis), lambda source, state: combine(state, take(source)), take(0)
    )


def combine_pairs(left_pair, right_pair):
    joined = jnp.maximum(left_pair[0], right_pair[0])
    left_scale = jnp.exp(left_pair[0] - joined)
    right_scale = jnp.exp(right_pair[0] - joined)
    numerator = left_pair[1] * left_scale[:, :, None] + right_pair[1] * right_scale[:, :, None]
    denom = left_pair[2] * left_scale + right_pair[2] * right_scale
    return (joined, numerator, denom)


MESH = pl.DeviceIdType.MESH
CHUNKS = 4
GROUP = 16
VMEM_SPEC = pl.BlockSpec(memory_space=pltpu.VMEM)


def two_terms(array):
    high = array.astype(BF16).astype(F32)
    return high, (array - high).astype(BF16).astype(F32)


def stream_kernel(
    scale,
    cell,
    norm,
    stab,
    queries,
    keys,
    values,
    in_gate,
    forget,
    new_cell,
    new_norm,
    new_stab,
    numer,
    small,
    lhs,
    rhs,
    keep_at,
):
    head, part = pl.program_id(0), pl.program_id(1)
    heads, blocks, seqs = stab.shape
    rows_k, cols_v = cell.shape[2:]
    rblk = rows_k // blocks
    per = cell.shape[0]

    @pl.when(part == 0)
    def _():
        pick = pl.ds(head, seqs, stride=heads)
        gate = in_gate[pl.ds(head, 1), :]
        carried = jax.nn.log_sigmoid(forget[pl.ds(head, 1), :]) + stab[head]
        fresh = jnp.maximum(carried, gate)
        top = jnp.max(fresh, axis=0, keepdims=True)
        new_stab[head] = fresh
        keep8 = jnp.exp(carried - fresh)
        keep_at[...] = keep8

        def spread(small8):
            rows = [jnp.broadcast_to(small8[b : b + 1, :], (rblk, seqs)) for b in range(blocks)]
            return jnp.concatenate(rows, axis=0).T

        write = spread(jnp.exp(gate - fresh)) * (keys[pick, :] * scale)
        weight = spread(jnp.exp(fresh - top)) * queries[pick, :]
        normal = spread(keep8) * norm[pick, :] + write
        new_norm[pick, :] = normal
        small[0, pl.ds(head, 1), :] = top
        small[1, pl.ds(head, 1), :] = jnp.sum((normal * weight).T, axis=0, keepdims=True)
        write_hi, write_lo = two_terms(write)
        weight_hi, weight_lo = two_terms(weight)
        value_hi, value_lo = two_terms(values[pick, :])
        zeros = jnp.zeros((GROUP, cols_v), F32)
        ones = jnp.ones((GROUP, cols_v), F32)
        for group in range(seqs // GROUP):
            rows = slice(group * GROUP, (group + 1) * GROUP)
            left = [write_hi[rows], write_hi[rows], write_lo[rows], weight_hi[rows], weight_lo[rows]]
            outer = [value_hi[rows], value_lo[rows], value_hi[rows], zeros, zeros]
            plain = [zeros, zeros, zeros, ones, ones]
            spare = rows_k // GROUP - len(left)
            stacked = jnp.concatenate(left + [zeros] * spare, axis=0)
            lhs[group] = stacked.T.astype(BF16)
            right = jnp.concatenate(
                [
                    jnp.concatenate(outer + [zeros] * spare, axis=0),
                    jnp.concatenate(plain + [zeros] * spare, axis=0),
                ],
                axis=1,
            )
            rhs[group] = right.astype(BF16)

    groups = per // GROUP
    keeps = keep_at[:, 0:per]
    for other in range(1, seqs // per):
        keeps = jnp.where(part == other, keep_at[:, other * per : (other + 1) * per], keeps)
    lane = lax.broadcasted_iota(jnp.int32, (rows_k, rows_k), 1) % GROUP
    for group in range(groups):
        left, right = lhs[part * groups + group], rhs[part * groups + group]
        for slot in range(GROUP):
            pair = group * GROUP + slot
            mine = jnp.where(lane == slot, left, jnp.zeros_like(left))
            spread = jnp.dot(mine, right, preferred_element_type=F32)
            kept = jnp.broadcast_to(keeps[:, pair : pair + 1], (blocks, cols_v))
            kept = jnp.concatenate(
                [jnp.broadcast_to(kept[b : b + 1, :], (rblk, cols_v)) for b in range(blocks)], axis=0
            )
            fresh_cell = kept * cell[pair, 0] + spread[:, :cols_v]
            new_cell[pair, 0] = fresh_cell
            numer[pl.ds((part * per + pair) * heads + head, 1), :] = jnp.sum(
                fresh_cell * spread[:, cols_v:], axis=0, keepdims=True
            )


def stream(cell, norm, stab, queries, keys, values, in_gate, forget):
    seqs, heads, rows_k, cols_v = cell.shape
    blocks = stab.shape[1]
    parts = seqs // PAIRS
    scale = (rows_k * lax.axis_size("row")) ** (-0.5)

    def whole(array):
        return pl.BlockSpec(array.shape, lambda h, p, n=len(array.shape): (0,) * n)

    tile = pl.BlockSpec((PAIRS, 1, rows_k, cols_v), lambda h, p: (p, h, 0, 0))
    out_shape = [
        jax.ShapeDtypeStruct(cell.shape, F32),
        jax.ShapeDtypeStruct(norm.shape, F32),
        jax.ShapeDtypeStruct(stab.shape, F32),
        jax.ShapeDtypeStruct((seqs * heads, cols_v), F32),
        jax.ShapeDtypeStruct((2, heads, seqs), F32),
    ]
    rest = (norm, stab, queries, keys, values, in_gate, forget)
    return pl.pallas_call(
        functools.partial(stream_kernel, scale),
        grid=(heads, parts),
        in_specs=[tile] + [whole(a) for a in rest],
        out_specs=[tile] + [whole(a) for a in out_shape[1:]],
        out_shape=out_shape,
        scratch_shapes=[
            pltpu.VMEM((seqs // GROUP, rows_k, rows_k), BF16),
            pltpu.VMEM((seqs // GROUP, rows_k, 2 * cols_v), BF16),
            pltpu.VMEM((blocks, seqs), F32),
        ],
        compiler_params=pltpu.CompilerParams(
            dimension_semantics=("arbitrary", "arbitrary"), vmem_limit_bytes=40 << 20
        ),
        cost_estimate=pl.CostEstimate(
            flops=200 * cell.size, bytes_accessed=8 * cell.size, transcendentals=0
        ),
    )(*(pltpu.with_memory_space_constraint(a, pltpu.HBM) for a in (cell, *rest)))


def tail_kernel(
    numer,
    small,
    logits,
    gain,
    weight,
    weight_far,
    layer_out,
    readout,
    numer_in,
    small_in,
    held,
    gate,
    gated,
    stats,
    stats_in,
    parts_out,
    parts_in,
    own,
    mine,
    mine_in,
    small_sems,
    row_sems,
    held_sems,
    stats_sems,
    parts_sems,
    mine_sems,
):
    row, hb, col = lax.axis_index("row"), lax.axis_index("hb"), lax.axis_index("col")
    cols, hbs = lax.axis_size("col"), lax.axis_size("hb")
    heads = small.shape[1]
    count, cols_v = numer.shape
    seqs = count // heads
    width = cols_v * cols
    per = seqs // CHUNKS
    depth, out_cols = weight.shape
    chunk = out_cols // cols
    across = 1 - row
    twin = hb + 1 - 2 * (hb % 2)
    peers = [(col + shift) % cols for shift in range(cols)]

    barrier = pltpu.get_barrier_semaphore()
    pl.semaphore_signal(barrier, inc=1, device_id={"row": across}, device_id_type=MESH)
    pl.semaphore_signal(barrier, inc=1, device_id={"hb": twin}, device_id_type=MESH)
    for shift in range(1, cols):
        pl.semaphore_signal(barrier, inc=1, device_id={"col": peers[shift]}, device_id_type=MESH)

    for chunk_at in range(CHUNKS):
        for seq in range(per):
            rows = pl.ds((chunk_at * per + seq) * heads, heads)
            gate[rows, :] = jax.nn.sigmoid(logits[rows, :]) * gain[...]

    pl.semaphore_wait(barrier, 1 + cols)

    def remote(source, target, sems, index, device):
        return pltpu.make_async_remote_copy(
            src_ref=source,
            dst_ref=target,
            send_sem=sems.at[(0,) + index],
            recv_sem=sems.at[(1,) + index],
            device_id=device,
            device_id_type=MESH,
        )

    small_copy = remote(small, small_in, small_sems, (0,), {"row": across})
    small_copy.start()
    row_copies = []
    for part in range(CHUNKS):
        rows = pl.ds(part * per * heads, per * heads)
        row_copies.append(
            remote(numer.at[rows, :], numer_in.at[rows, :], row_sems, (part,), {"row": across})
        )
        row_copies[part].start()
    twins = [
        remote(source, held.at[slot], held_sems, (slot,), {"hb": twin})
        for slot, source in enumerate((weight, weight_far))
    ]
    for copy in twins:
        copy.start()

    small_copy.wait()
    joined = jnp.maximum(small[0], small_in[0])
    own_scale = jnp.exp(small[0] - joined)
    other_scale = jnp.exp(small_in[0] - joined)
    denom = small[1] * own_scale + small_in[1] * other_scale
    bound = jnp.maximum(jnp.abs(denom), jnp.exp(-joined))
    own_scale = own_scale / bound
    other_scale = other_scale / bound
    lane = lax.broadcasted_iota(jnp.int32, (heads, cols_v), 1)

    blocks = (weight, weight_far, held.at[0], held.at[1])
    stats_copies, parts_copies, mine_copies = {}, {}, {}

    def combine(part):
        row_copies[part].wait()
        sums = jnp.zeros((heads, cols_v), F32)
        squares = sums
        for seq in range(per):
            at = part * per + seq
            rows = pl.ds(at * heads, heads)
            value = (
                numer[rows, :] * own_scale[:, at : at + 1]
                + numer_in[rows, :] * other_scale[:, at : at + 1]
            )
            readout[rows, :] = value
            sums = jnp.where(lane == seq, jnp.sum(value, axis=1, keepdims=True), sums)
            squares = jnp.where(lane == seq, jnp.sum(value * value, axis=1, keepdims=True), squares)
        stats[part, 0] = sums
        stats[part, 1] = squares
        for shift in range(1, cols):
            copy = remote(
                stats.at[part],
                stats_in.at[part, shift - 1],
                stats_sems,
                (part, shift - 1),
                {"col": peers[shift]},
            )
            copy.start()
            stats_copies[part, shift] = copy

    def project(part):
        for shift in range(1, cols):
            stats_copies[part, shift].wait()
        total = functools.reduce(
            lambda a, b: a + b, [stats_in[part, shift] for shift in range(cols - 1)], stats[part]
        )
        mean = total[0] / width
        rate = lax.rsqrt(total[1] / width - mean * mean + 1e-06)
        for seq in range(per):
            rows = pl.ds((part * per + seq) * heads, heads)
            gated[rows, :] = (
                (readout[rows, :] - mean[:, seq : seq + 1]) * rate[:, seq : seq + 1] * gate[rows, :]
            )
        if part == 0:
            for copy in twins:
                copy.wait()
        owners = [hb, (hb + 2) % hbs, twin, (twin + 2) % hbs]
        lefts = []
        for owner in owners:
            pieces = [
                gated[pl.ds(part * per * heads + owner * (depth // cols_v) + at, per, stride=heads), :]
                for at in range(depth // cols_v)
            ]
            lefts.append(jnp.concatenate(pieces, axis=1).astype(BF16))
        for shift in list(range(1, cols)) + [0]:
            start = pl.multiple_of(peers[shift] * chunk, chunk)
            term = None
            for slot, left in enumerate(lefts):
                block = blocks[slot][:, pl.ds(start, chunk)]
                product = jnp.dot(left, block, preferred_element_type=F32)
                term = product if term is None else term + product
            if shift == 0:
                own[part] = term
                continue
            parts_out[part, shift - 1] = term.astype(BF16)
            copy = remote(
                parts_out.at[part, shift - 1],
                parts_in.at[part, shift - 1],
                parts_sems,
                (part, shift - 1),
                {"col": peers[shift]},
            )
            copy.start()
            parts_copies[part, shift] = copy

    def gather(part):
        total = own[part]
        for shift in range(1, cols):
            parts_copies[part, shift].wait()
            total = total + parts_in[part, shift - 1].astype(F32)
        total = total.astype(BF16)
        mine[part] = total
        for shift in range(1, cols):
            copy = remote(
                mine.at[part],
                mine_in.at[part, shift - 1],
                mine_sems,
                (part, shift - 1),
                {"col": peers[shift]},
            )
            copy.start()
            mine_copies[part, shift] = copy
        start = pl.multiple_of(col * chunk, chunk)
        layer_out[pl.ds(part * per, per), pl.ds(start, chunk)] = total.astype(F32)

    def finish(part):
        for shift in range(1, cols):
            mine_copies[part, shift].wait()
            start = pl.multiple_of(((col + cols - shift) % cols) * chunk, chunk)
            layer_out[pl.ds(part * per, per), pl.ds(start, chunk)] = mine_in[
                part, shift - 1
            ].astype(F32)

    steps = ((combine, 0), (project, 1), (gather, 2), (finish, 3))
    for tick in range(CHUNKS + 3):
        for step, delay in steps:
            if 0 <= tick - delay < CHUNKS:
                step(tick - delay)


def tail(numer, small, logits, gain, weight, weight_far):
    cols = lax.axis_size("col")
    count, cols_v = numer.shape
    heads, seqs = small.shape[1:]
    depth, out_cols = weight.shape
    per = seqs // CHUNKS
    chunk = out_cols // cols
    sems = lambda *shape: pltpu.SemaphoreType.DMA((2,) + shape)
    return pl.pallas_call(
        tail_kernel,
        in_specs=[VMEM_SPEC] * 6,
        out_specs=[VMEM_SPEC] * 2,
        out_shape=[
            jax.ShapeDtypeStruct((seqs, out_cols), F32),
            jax.ShapeDtypeStruct((count, cols_v), F32),
        ],
        scratch_shapes=[
            pltpu.VMEM((count, cols_v), F32),
            pltpu.VMEM(small.shape, F32),
            pltpu.VMEM((2, depth, out_cols), BF16),
            pltpu.VMEM((count, cols_v), F32),
            pltpu.VMEM((count, cols_v), F32),
            pltpu.VMEM((CHUNKS, 2, heads, cols_v), F32),
            pltpu.VMEM((CHUNKS, cols - 1, 2, heads, cols_v), F32),
            pltpu.VMEM((CHUNKS, cols - 1, per, chunk), BF16),
            pltpu.VMEM((CHUNKS, cols - 1, per, chunk), BF16),
            pltpu.VMEM((CHUNKS, per, chunk), F32),
            pltpu.VMEM((CHUNKS, per, chunk), BF16),
            pltpu.VMEM((CHUNKS, cols - 1, per, chunk), BF16),
            sems(1),
            sems(CHUNKS),
            sems(2),
            sems(CHUNKS, cols - 1),
            sems(CHUNKS, cols - 1),
            sems(CHUNKS, cols - 1),
        ],
        compiler_params=pltpu.CompilerParams(
            vmem_limit_bytes=24 << 20, collective_id=0, has_side_effects=True
        ),
        cost_estimate=pl.CostEstimate(
            flops=2 * seqs * 4 * depth * out_cols,
            bytes_accessed=8 * depth * out_cols,
            transcendentals=0,
        ),
    )(numer, small, logits, gain, weight, weight_far)


def fused(
    cell_state,
    normalizer,
    stabilizer,
    queries,
    key_vectors,
    token_value_vectors,
    input_gate,
    forget_gate,
    output_gate_logits,
    norm_gain,
    out_weight,
):
    seqs, heads, rows_k, cols_v = cell_state.shape
    flat = lambda a: a.reshape((seqs * heads,) + a.shape[2:])
    weight = out_weight.reshape(-1, out_weight.shape[2])
    weight_far = lax.ppermute(weight, "hb", [(i, (i + 2) % 4) for i in range(4)])
    refreshed_cell, new_normal, fresh, numer, small = stream(
        cell_state,
        flat(normalizer),
        stabilizer.transpose(1, 2, 0),
        flat(queries),
        flat(key_vectors),
        flat(token_value_vectors),
        input_gate.T,
        forget_gate.T,
    )
    layer_out, readout = tail(
        numer, small, flat(output_gate_logits), norm_gain, weight, weight_far
    )
    return (
        layer_out,
        readout.reshape(seqs, heads, cols_v),
        refreshed_cell,
        new_normal.reshape(normalizer.shape),
        fresh.transpose(2, 0, 1),
    )


def fits(cell_state, out_weight):
    seqs, heads, rows_k, cols_v = cell_state.shape
    sizes = tuple(lax.axis_size(axis) for axis in ("hb", "row", "col"))
    return (
        sizes == (4, 2, 4)
        and heads == 8
        and rows_k == cols_v == 128
        and seqs % max(PAIRS, CHUNKS * GROUP) == 0
        and seqs <= 128
        and out_weight.shape[0] * sizes[0] == heads
        and out_weight.shape[2] % (128 * sizes[2]) == 0
    )


def local(
    cell_state,
    normalizer,
    stabilizer,
    queries,
    key_vectors,
    token_value_vectors,
    input_gate,
    forget_gate,
    output_gate_logits,
    norm_gain,
    out_weight,
):
    if fits(cell_state, out_weight):
        return fused(
            cell_state,
            normalizer,
            stabilizer,
            queries,
            key_vectors,
            token_value_vectors,
            input_gate,
            forget_gate,
            output_gate_logits,
            norm_gain,
            out_weight,
        )
    seqs, heads, rows_k, cols_v = cell_state.shape
    rblk = rows_k // stabilizer.shape[2]
    scale = (rows_k * lax.axis_size("row")) ** (-0.5)
    carried = jax.nn.log_sigmoid(forget_gate)[:, :, None] + stabilizer
    fresh = jnp.maximum(carried, input_gate[:, :, None])
    keep8 = jnp.exp(carried - fresh)
    admit8 = jnp.exp(input_gate[:, :, None] - fresh)
    local_top = jnp.max(fresh, axis=2)
    keep = jnp.repeat(keep8, rblk, axis=2)
    write = jnp.repeat(admit8, rblk, axis=2) * key_vectors * scale
    refreshed_cell = (
        keep[:, :, :, None] * cell_state
        + write[:, :, :, None] * token_value_vectors[:, :, None, :]
    )
    new_normal = keep * normalizer + write
    weight = jnp.repeat(jnp.exp(fresh - local_top[:, :, None]), rblk, axis=2) * queries
    numerator = jnp.einsum(
        "bhkv,bhk->bhv", refreshed_cell, weight, precision=lax.Precision.HIGHEST
    )
    denom = jnp.sum(new_normal * weight, axis=2)
    top, numerator, denom = combined_all((local_top, numerator, denom), "row", combine_pairs)
    readout = numerator / jnp.maximum(jnp.abs(denom), jnp.exp(-top))[:, :, None]
    stats = jnp.stack([jnp.sum(readout, axis=2), jnp.sum(readout * readout, axis=2)])
    cols = lax.axis_size("col")
    sums = lax.psum(stats, "col")
    mean = sums[0] / (cols_v * cols)
    var = sums[1] / (cols_v * cols) - mean * mean
    normed = (readout - mean[:, :, None]) * lax.rsqrt(var + 1e-06)[:, :, None]
    gated = (normed * norm_gain * jax.nn.sigmoid(output_gate_logits)).astype(BF16)
    gated = gated.reshape(seqs, -1)
    out_cols = out_weight.shape[2]
    partial_value = jnp.dot(
        gated,
        lax.all_gather(out_weight, "hb", axis=0, tiled=True).reshape(-1, out_cols),
        preferred_element_type=F32,
    )
    layer_out = lax.psum(partial_value, "col")
    return (layer_out, readout, refreshed_cell, new_normal, fresh)


def solution(mesh):
    placed = (
        P("hb", None, "row", "col"),
        P("hb", None, "row"),
        P("hb", None, "row"),
        P("hb", None, "row"),
        P("hb", None, "row"),
        P("hb", None, "col"),
        P("hb", None),
        P("hb", None),
        P("hb", None, "col"),
        P(None, "col"),
        P("hb", "col", "row"),
    )
    return jax.shard_map(
        local,
        mesh=mesh,
        in_specs=placed,
        out_specs=(
            P("hb", "row"),
            P("hb", None, "col"),
            P("hb", None, "row", "col"),
            P("hb", None, "row"),
            P("hb", None, "row"),
        ),
        check_vma=False,
    )
```

```python
import functools

import jax
import jax.numpy as jnp
from jax import lax
from jax.experimental import pallas as pl
from jax.experimental.pallas import tpu as pltpu
from jax.sharding import PartitionSpec as P

PAIRS = 64
F32 = jnp.float32
BF16 = jnp.bfloat16


def combined_all(part, axis, combine):
    gathered = jax.tree.map(lambda a: lax.all_gather(a, axis), part)

    def take(source):
        return jax.tree.map(lambda a: lax.dynamic_index_in_dim(a, source, 0, False), gathered)

    return lax.fori_loop(
        1, lax.axis_size(axis), lambda source, state: combine(state, take(source)), take(0)
    )


def combine_pairs(left_pair, right_pair):
    joined = jnp.maximum(left_pair[0], right_pair[0])
    left_scale = jnp.exp(left_pair[0] - joined)
    right_scale = jnp.exp(right_pair[0] - joined)
    numerator = left_pair[1] * left_scale[:, :, None] + right_pair[1] * right_scale[:, :, None]
    denom = left_pair[2] * left_scale + right_pair[2] * right_scale
    return (joined, numerator, denom)


MESH = pl.DeviceIdType.MESH
CHUNKS = 4
GROUP = 16
AHEAD = 3
VMEM_SPEC = pl.BlockSpec(memory_space=pltpu.VMEM)
HBM_SPEC = pl.BlockSpec(memory_space=pltpu.HBM)


def two_terms(array):
    high = array.astype(BF16).astype(F32)
    return high, (array - high).astype(BF16).astype(F32)


def stream_kernel(
    scale,
    cell,
    norm_hbm,
    stab_hbm,
    queries_hbm,
    keys_hbm,
    values_hbm,
    in_gate_hbm,
    forget_hbm,
    new_cell,
    new_norm,
    new_stab,
    numer,
    small,
    norm,
    stab,
    queries,
    keys,
    values,
    in_gate,
    forget,
    tiles,
    lhs,
    rhs,
    keep_at,
    small_sems,
    in_sems,
    out_sems,
):
    head, part = pl.program_id(0), pl.program_id(1)
    heads, blocks, seqs = stab.shape
    count, per, rows_k, cols_v = tiles.shape
    parts = count // heads
    rblk = rows_k // blocks

    def fetch(at):
        source = cell.at[pl.ds((at % parts) * per, per), at // parts]
        return pltpu.make_async_copy(source, tiles.at[at], in_sems.at[at])

    def flush(at):
        target = new_cell.at[pl.ds((at % parts) * per, per), at // parts]
        return pltpu.make_async_copy(tiles.at[at], target, out_sems.at[at])

    @pl.when((head == 0) & (part == 0))
    def _():
        pairs = (
            (stab_hbm, stab),
            (in_gate_hbm, in_gate),
            (forget_hbm, forget),
            (norm_hbm, norm),
            (queries_hbm, queries),
            (keys_hbm, keys),
            (values_hbm, values),
        )
        copies = [
            pltpu.make_async_copy(source, target, small_sems.at[index])
            for index, (source, target) in enumerate(pairs)
        ]
        for copy in copies:
            copy.start()
        for ahead in range(AHEAD):
            fetch(ahead).start()
        for copy in copies:
            copy.wait()

    @pl.when(part == 0)
    def _():
        pick = pl.ds(head, seqs, stride=heads)
        gate = in_gate[pl.ds(head, 1), :]
        carried = jax.nn.log_sigmoid(forget[pl.ds(head, 1), :]) + stab[head]
        fresh = jnp.maximum(carried, gate)
        top = jnp.max(fresh, axis=0, keepdims=True)
        new_stab[head] = fresh
        keep8 = jnp.exp(carried - fresh)
        keep_at[...] = keep8

        def spread(small8):
            rows = [jnp.broadcast_to(small8[b : b + 1, :], (rblk, seqs)) for b in range(blocks)]
            return jnp.concatenate(rows, axis=0).T

        write = spread(jnp.exp(gate - fresh)) * (keys[pick, :] * scale)
        weight = spread(jnp.exp(fresh - top)) * queries[pick, :]
        normal = spread(keep8) * norm[pick, :] + write
        new_norm[pick, :] = normal
        small[0, pl.ds(head, 1), :] = top
        small[1, pl.ds(head, 1), :] = jnp.sum((normal * weight).T, axis=0, keepdims=True)
        write_hi, write_lo = two_terms(write)
        weight_hi, weight_lo = two_terms(weight)
        value_hi, value_lo = two_terms(values[pick, :])
        zeros = jnp.zeros((GROUP, cols_v), F32)
        ones = jnp.ones((GROUP, cols_v), F32)
        for group in range(seqs // GROUP):
            rows = slice(group * GROUP, (group + 1) * GROUP)
            left = [write_hi[rows], write_hi[rows], write_lo[rows], weight_hi[rows], weight_lo[rows]]
            outer = [value_hi[rows], value_lo[rows], value_hi[rows], zeros, zeros]
            plain = [zeros, zeros, zeros, ones, ones]
            spare = rows_k // GROUP - len(left)
            stacked = jnp.concatenate(left + [zeros] * spare, axis=0)
            lhs[group] = stacked.T.astype(BF16)
            right = jnp.concatenate(
                [
                    jnp.concatenate(outer + [zeros] * spare, axis=0),
                    jnp.concatenate(plain + [zeros] * spare, axis=0),
                ],
                axis=1,
            )
            rhs[group] = right.astype(BF16)

    at = head * parts + part
    groups = per // GROUP
    keeps = keep_at[:, 0:per]
    for other in range(1, parts):
        keeps = jnp.where(part == other, keep_at[:, other * per : (other + 1) * per], keeps)
    lane = lax.broadcasted_iota(jnp.int32, (rows_k, rows_k), 1) % GROUP

    @pl.when(at + AHEAD < count)
    def _():
        fetch(at + AHEAD).start()

    fetch(at).wait()
    for group in range(groups):
        left, right = lhs[part * groups + group], rhs[part * groups + group]
        for slot in range(GROUP):
            pair = group * GROUP + slot
            mine = jnp.where(lane == slot, left, jnp.zeros_like(left))
            spread = jnp.dot(mine, right, preferred_element_type=F32)
            kept = jnp.broadcast_to(keeps[:, pair : pair + 1], (blocks, cols_v))
            kept = jnp.concatenate(
                [jnp.broadcast_to(kept[b : b + 1, :], (rblk, cols_v)) for b in range(blocks)], axis=0
            )
            fresh_cell = kept * tiles[at, pair] + spread[:, :cols_v]
            tiles[at, pair] = fresh_cell
            numer[pl.ds((part * per + pair) * heads + head, 1), :] = jnp.sum(
                fresh_cell * spread[:, cols_v:], axis=0, keepdims=True
            )
    flush(at).start()

    @pl.when(at == count - 1)
    def _():
        for done in range(count):
            flush(done).wait()


def stream(cell, norm, stab, queries, keys, values, in_gate, forget):
    seqs, heads, rows_k, cols_v = cell.shape
    blocks = stab.shape[1]
    parts = seqs // PAIRS
    scale = (rows_k * lax.axis_size("row")) ** (-0.5)

    def whole(array):
        return pl.BlockSpec(array.shape, lambda h, p, n=len(array.shape): (0,) * n)

    out_shape = [
        jax.ShapeDtypeStruct(cell.shape, F32),
        jax.ShapeDtypeStruct(norm.shape, F32),
        jax.ShapeDtypeStruct(stab.shape, F32),
        jax.ShapeDtypeStruct((seqs * heads, cols_v), F32),
        jax.ShapeDtypeStruct((2, heads, seqs), F32),
    ]
    rest = (norm, stab, queries, keys, values, in_gate, forget)
    args = [pltpu.with_memory_space_constraint(a, pltpu.HBM) for a in (cell, *rest)]
    return pl.pallas_call(
        functools.partial(stream_kernel, scale),
        grid=(heads, parts),
        in_specs=[HBM_SPEC] * len(args),
        out_specs=[HBM_SPEC] + [whole(a) for a in out_shape[1:]],
        out_shape=out_shape,
        scratch_shapes=[pltpu.VMEM(a.shape, F32) for a in rest]
        + [
            pltpu.VMEM((heads * parts, PAIRS, rows_k, cols_v), F32),
            pltpu.VMEM((seqs // GROUP, rows_k, rows_k), BF16),
            pltpu.VMEM((seqs // GROUP, rows_k, 2 * cols_v), BF16),
            pltpu.VMEM((blocks, seqs), F32),
            pltpu.SemaphoreType.DMA((len(rest),)),
            pltpu.SemaphoreType.DMA((heads * parts,)),
            pltpu.SemaphoreType.DMA((heads * parts,)),
        ],
        compiler_params=pltpu.CompilerParams(
            dimension_semantics=("arbitrary", "arbitrary"), vmem_limit_bytes=44 << 20
        ),
        cost_estimate=pl.CostEstimate(
            flops=200 * cell.size, bytes_accessed=8 * cell.size, transcendentals=0
        ),
    )(*args)


def tail_kernel(
    numer,
    small,
    logits,
    gain,
    weight,
    weight_far,
    layer_out,
    readout,
    numer_in,
    small_in,
    held,
    gate,
    gated,
    stats,
    stats_in,
    parts_out,
    parts_in,
    own,
    mine,
    mine_in,
    small_sems,
    row_sems,
    held_sems,
    stats_sems,
    parts_sems,
    mine_sems,
):
    row, hb, col = lax.axis_index("row"), lax.axis_index("hb"), lax.axis_index("col")
    cols, hbs = lax.axis_size("col"), lax.axis_size("hb")
    heads = small.shape[1]
    count, cols_v = numer.shape
    seqs = count // heads
    width = cols_v * cols
    per = seqs // CHUNKS
    depth, out_cols = weight.shape
    chunk = out_cols // cols
    across = 1 - row
    twin = hb + 1 - 2 * (hb % 2)
    peers = [(col + shift) % cols for shift in range(cols)]

    barrier = pltpu.get_barrier_semaphore()
    pl.semaphore_signal(barrier, inc=1, device_id={"row": across}, device_id_type=MESH)
    pl.semaphore_signal(barrier, inc=1, device_id={"hb": twin}, device_id_type=MESH)
    for shift in range(1, cols):
        pl.semaphore_signal(barrier, inc=1, device_id={"col": peers[shift]}, device_id_type=MESH)

    for chunk_at in range(CHUNKS):
        for seq in range(per):
            rows = pl.ds((chunk_at * per + seq) * heads, heads)
            gate[rows, :] = jax.nn.sigmoid(logits[rows, :]) * gain[...]

    pl.semaphore_wait(barrier, 1 + cols)

    def remote(source, target, sems, index, device):
        return pltpu.make_async_remote_copy(
            src_ref=source,
            dst_ref=target,
            send_sem=sems.at[(0,) + index],
            recv_sem=sems.at[(1,) + index],
            device_id=device,
            device_id_type=MESH,
        )

    small_copy = remote(small, small_in, small_sems, (0,), {"row": across})
    small_copy.start()
    row_copies = []
    for part in range(CHUNKS):
        rows = pl.ds(part * per * heads, per * heads)
        row_copies.append(
            remote(numer.at[rows, :], numer_in.at[rows, :], row_sems, (part,), {"row": across})
        )
        row_copies[part].start()
    twins = [
        remote(source, held.at[slot], held_sems, (slot,), {"hb": twin})
        for slot, source in enumerate((weight, weight_far))
    ]
    for copy in twins:
        copy.start()

    small_copy.wait()
    joined = jnp.maximum(small[0], small_in[0])
    own_scale = jnp.exp(small[0] - joined)
    other_scale = jnp.exp(small_in[0] - joined)
    denom = small[1] * own_scale + small_in[1] * other_scale
    bound = jnp.maximum(jnp.abs(denom), jnp.exp(-joined))
    own_scale = own_scale / bound
    other_scale = other_scale / bound
    lane = lax.broadcasted_iota(jnp.int32, (heads, cols_v), 1)

    blocks = (weight, weight_far, held.at[0], held.at[1])
    stats_copies, parts_copies, mine_copies = {}, {}, {}

    def combine(part):
        row_copies[part].wait()
        sums = jnp.zeros((heads, cols_v), F32)
        squares = sums
        for seq in range(per):
            at = part * per + seq
            rows = pl.ds(at * heads, heads)
            value = (
                numer[rows, :] * own_scale[:, at : at + 1]
                + numer_in[rows, :] * other_scale[:, at : at + 1]
            )
            readout[rows, :] = value
            sums = jnp.where(lane == seq, jnp.sum(value, axis=1, keepdims=True), sums)
            squares = jnp.where(lane == seq, jnp.sum(value * value, axis=1, keepdims=True), squares)
        stats[part, 0] = sums
        stats[part, 1] = squares
        for shift in range(1, cols):
            copy = remote(
                stats.at[part],
                stats_in.at[part, shift - 1],
                stats_sems,
                (part, shift - 1),
                {"col": peers[shift]},
            )
            copy.start()
            stats_copies[part, shift] = copy

    def project(part):
        for shift in range(1, cols):
            stats_copies[part, shift].wait()
        total = functools.reduce(
            lambda a, b: a + b, [stats_in[part, shift] for shift in range(cols - 1)], stats[part]
        )
        mean = total[0] / width
        rate = lax.rsqrt(total[1] / width - mean * mean + 1e-06)
        for seq in range(per):
            rows = pl.ds((part * per + seq) * heads, heads)
            gated[rows, :] = (
                (readout[rows, :] - mean[:, seq : seq + 1]) * rate[:, seq : seq + 1] * gate[rows, :]
            )
        if part == 0:
            for copy in twins:
                copy.wait()
        owners = [hb, (hb + 2) % hbs, twin, (twin + 2) % hbs]
        lefts = []
        for owner in owners:
            pieces = [
                gated[pl.ds(part * per * heads + owner * (depth // cols_v) + at, per, stride=heads), :]
                for at in range(depth // cols_v)
            ]
            lefts.append(jnp.concatenate(pieces, axis=1).astype(BF16))
        for shift in list(range(1, cols)) + [0]:
            start = pl.multiple_of(peers[shift] * chunk, chunk)
            term = None
            for slot, left in enumerate(lefts):
                block = blocks[slot][:, pl.ds(start, chunk)]
                product = jnp.dot(left, block, preferred_element_type=F32)
                term = product if term is None else term + product
            if shift == 0:
                own[part] = term
                continue
            parts_out[part, shift - 1] = term.astype(BF16)
            copy = remote(
                parts_out.at[part, shift - 1],
                parts_in.at[part, shift - 1],
                parts_sems,
                (part, shift - 1),
                {"col": peers[shift]},
            )
            copy.start()
            parts_copies[part, shift] = copy

    def gather(part):
        total = own[part]
        for shift in range(1, cols):
            parts_copies[part, shift].wait()
            total = total + parts_in[part, shift - 1].astype(F32)
        total = total.astype(BF16)
        mine[part] = total
        for shift in range(1, cols):
            copy = remote(
                mine.at[part],
                mine_in.at[part, shift - 1],
                mine_sems,
                (part, shift - 1),
                {"col": peers[shift]},
            )
            copy.start()
            mine_copies[part, shift] = copy
        start = pl.multiple_of(col * chunk, chunk)
        layer_out[pl.ds(part * per, per), pl.ds(start, chunk)] = total.astype(F32)

    def finish(part):
        for shift in range(1, cols):
            mine_copies[part, shift].wait()
            start = pl.multiple_of(((col + cols - shift) % cols) * chunk, chunk)
            layer_out[pl.ds(part * per, per), pl.ds(start, chunk)] = mine_in[
                part, shift - 1
            ].astype(F32)

    steps = ((combine, 0), (project, 1), (gather, 2), (finish, 3))
    for tick in range(CHUNKS + 3):
        for step, delay in steps:
            if 0 <= tick - delay < CHUNKS:
                step(tick - delay)


def tail(numer, small, logits, gain, weight, weight_far):
    cols = lax.axis_size("col")
    count, cols_v = numer.shape
    heads, seqs = small.shape[1:]
    depth, out_cols = weight.shape
    per = seqs // CHUNKS
    chunk = out_cols // cols
    sems = lambda *shape: pltpu.SemaphoreType.DMA((2,) + shape)
    return pl.pallas_call(
        tail_kernel,
        in_specs=[VMEM_SPEC] * 6,
        out_specs=[VMEM_SPEC] * 2,
        out_shape=[
            jax.ShapeDtypeStruct((seqs, out_cols), F32),
            jax.ShapeDtypeStruct((count, cols_v), F32),
        ],
        scratch_shapes=[
            pltpu.VMEM((count, cols_v), F32),
            pltpu.VMEM(small.shape, F32),
            pltpu.VMEM((2, depth, out_cols), BF16),
            pltpu.VMEM((count, cols_v), F32),
            pltpu.VMEM((count, cols_v), F32),
            pltpu.VMEM((CHUNKS, 2, heads, cols_v), F32),
            pltpu.VMEM((CHUNKS, cols - 1, 2, heads, cols_v), F32),
            pltpu.VMEM((CHUNKS, cols - 1, per, chunk), BF16),
            pltpu.VMEM((CHUNKS, cols - 1, per, chunk), BF16),
            pltpu.VMEM((CHUNKS, per, chunk), F32),
            pltpu.VMEM((CHUNKS, per, chunk), BF16),
            pltpu.VMEM((CHUNKS, cols - 1, per, chunk), BF16),
            sems(1),
            sems(CHUNKS),
            sems(2),
            sems(CHUNKS, cols - 1),
            sems(CHUNKS, cols - 1),
            sems(CHUNKS, cols - 1),
        ],
        compiler_params=pltpu.CompilerParams(
            vmem_limit_bytes=24 << 20, collective_id=0, has_side_effects=True
        ),
        cost_estimate=pl.CostEstimate(
            flops=2 * seqs * 4 * depth * out_cols,
            bytes_accessed=8 * depth * out_cols,
            transcendentals=0,
        ),
    )(numer, small, logits, gain, weight, weight_far)


def settle_kernel(layer_out, readout, layer_hbm, readout_hbm, sems):
    copies = [
        pltpu.make_async_copy(source, target, sems.at[index])
        for index, (source, target) in enumerate(((layer_out, layer_hbm), (readout, readout_hbm)))
    ]
    for copy in copies:
        copy.start()
    for copy in copies:
        copy.wait()


def settle(layer_out, readout):
    return pl.pallas_call(
        settle_kernel,
        in_specs=[VMEM_SPEC] * 2,
        out_specs=[pl.BlockSpec(memory_space=pl.ANY)] * 2,
        out_shape=[jax.ShapeDtypeStruct(a.shape, F32) for a in (layer_out, readout)],
        scratch_shapes=[pltpu.SemaphoreType.DMA((2,))],
        compiler_params=pltpu.CompilerParams(vmem_limit_bytes=4 << 20),
    )(layer_out, readout)


def fused(
    cell_state,
    normalizer,
    stabilizer,
    queries,
    key_vectors,
    token_value_vectors,
    input_gate,
    forget_gate,
    output_gate_logits,
    norm_gain,
    out_weight,
):
    seqs, heads, rows_k, cols_v = cell_state.shape
    flat = lambda a: a.reshape((seqs * heads,) + a.shape[2:])
    weight = out_weight.reshape(-1, out_weight.shape[2])
    weight_far = lax.ppermute(weight, "hb", [(i, (i + 2) % 4) for i in range(4)])
    refreshed_cell, new_normal, fresh, numer, small = stream(
        cell_state,
        flat(normalizer),
        stabilizer.transpose(1, 2, 0),
        flat(queries),
        flat(key_vectors),
        flat(token_value_vectors),
        input_gate.T,
        forget_gate.T,
    )
    layer_out, readout = settle(
        *tail(numer, small, flat(output_gate_logits), norm_gain, weight, weight_far)
    )
    return (
        layer_out,
        readout.reshape(seqs, heads, cols_v),
        refreshed_cell,
        new_normal.reshape(normalizer.shape),
        fresh.transpose(2, 0, 1),
    )


def fits(cell_state, out_weight):
    seqs, heads, rows_k, cols_v = cell_state.shape
    sizes = tuple(lax.axis_size(axis) for axis in ("hb", "row", "col"))
    return (
        sizes == (4, 2, 4)
        and heads == 8
        and rows_k == cols_v == 128
        and seqs % max(PAIRS, CHUNKS * GROUP) == 0
        and seqs <= 128
        and out_weight.shape[0] * sizes[0] == heads
        and out_weight.shape[2] % (128 * sizes[2]) == 0
    )


def local(
    cell_state,
    normalizer,
    stabilizer,
    queries,
    key_vectors,
    token_value_vectors,
    input_gate,
    forget_gate,
    output_gate_logits,
    norm_gain,
    out_weight,
):
    if fits(cell_state, out_weight):
        return fused(
            cell_state,
            normalizer,
            stabilizer,
            queries,
            key_vectors,
            token_value_vectors,
            input_gate,
            forget_gate,
            output_gate_logits,
            norm_gain,
            out_weight,
        )
    seqs, heads, rows_k, cols_v = cell_state.shape
    rblk = rows_k // stabilizer.shape[2]
    scale = (rows_k * lax.axis_size("row")) ** (-0.5)
    carried = jax.nn.log_sigmoid(forget_gate)[:, :, None] + stabilizer
    fresh = jnp.maximum(carried, input_gate[:, :, None])
    keep8 = jnp.exp(carried - fresh)
    admit8 = jnp.exp(input_gate[:, :, None] - fresh)
    local_top = jnp.max(fresh, axis=2)
    keep = jnp.repeat(keep8, rblk, axis=2)
    write = jnp.repeat(admit8, rblk, axis=2) * key_vectors * scale
    refreshed_cell = (
        keep[:, :, :, None] * cell_state
        + write[:, :, :, None] * token_value_vectors[:, :, None, :]
    )
    new_normal = keep * normalizer + write
    weight = jnp.repeat(jnp.exp(fresh - local_top[:, :, None]), rblk, axis=2) * queries
    numerator = jnp.einsum(
        "bhkv,bhk->bhv", refreshed_cell, weight, precision=lax.Precision.HIGHEST
    )
    denom = jnp.sum(new_normal * weight, axis=2)
    top, numerator, denom = combined_all((local_top, numerator, denom), "row", combine_pairs)
    readout = numerator / jnp.maximum(jnp.abs(denom), jnp.exp(-top))[:, :, None]
    stats = jnp.stack([jnp.sum(readout, axis=2), jnp.sum(readout * readout, axis=2)])
    cols = lax.axis_size("col")
    sums = lax.psum(stats, "col")
    mean = sums[0] / (cols_v * cols)
    var = sums[1] / (cols_v * cols) - mean * mean
    normed = (readout - mean[:, :, None]) * lax.rsqrt(var + 1e-06)[:, :, None]
    gated = (normed * norm_gain * jax.nn.sigmoid(output_gate_logits)).astype(BF16)
    gated = gated.reshape(seqs, -1)
    out_cols = out_weight.shape[2]
    partial_value = jnp.dot(
        gated,
        lax.all_gather(out_weight, "hb", axis=0, tiled=True).reshape(-1, out_cols),
        preferred_element_type=F32,
    )
    layer_out = lax.psum(partial_value, "col")
    return (layer_out, readout, refreshed_cell, new_normal, fresh)


def solution(mesh):
    placed = (
        P("hb", None, "row", "col"),
        P("hb", None, "row"),
        P("hb", None, "row"),
        P("hb", None, "row"),
        P("hb", None, "row"),
        P("hb", None, "col"),
        P("hb", None),
        P("hb", None),
        P("hb", None, "col"),
        P(None, "col"),
        P("hb", "col", "row"),
    )
    return jax.shard_map(
        local,
        mesh=mesh,
        in_specs=placed,
        out_specs=(
            P("hb", "row"),
            P("hb", None, "col"),
            P("hb", None, "row", "col"),
            P("hb", None, "row"),
            P("hb", None, "row"),
        ),
        check_vma=False,
    )
```

```python
import functools

import jax
import jax.numpy as jnp
from jax import lax
from jax.experimental import pallas as pl
from jax.experimental.pallas import tpu as pltpu
from jax.sharding import PartitionSpec as P

PAIRS = 64
F32 = jnp.float32
BF16 = jnp.bfloat16


def combined_all(part, axis, combine):
    gathered = jax.tree.map(lambda a: lax.all_gather(a, axis), part)

    def take(source):
        return jax.tree.map(lambda a: lax.dynamic_index_in_dim(a, source, 0, False), gathered)

    return lax.fori_loop(
        1, lax.axis_size(axis), lambda source, state: combine(state, take(source)), take(0)
    )


def combine_pairs(left_pair, right_pair):
    joined = jnp.maximum(left_pair[0], right_pair[0])
    left_scale = jnp.exp(left_pair[0] - joined)
    right_scale = jnp.exp(right_pair[0] - joined)
    numerator = left_pair[1] * left_scale[:, :, None] + right_pair[1] * right_scale[:, :, None]
    denom = left_pair[2] * left_scale + right_pair[2] * right_scale
    return (joined, numerator, denom)


MESH = pl.DeviceIdType.MESH
SPLIT = (2, 2)
CHUNKS = len(SPLIT)
GROUP = 16
AHEAD = 3
VMEM_SPEC = pl.BlockSpec(memory_space=pltpu.VMEM)
HBM_SPEC = pl.BlockSpec(memory_space=pltpu.HBM)


def two_terms(array):
    high = array.astype(BF16).astype(F32)
    return high, (array - high).astype(BF16).astype(F32)


def stream_kernel(
    scale,
    cell,
    norm_hbm,
    stab_hbm,
    queries_hbm,
    keys_hbm,
    values_hbm,
    in_gate_hbm,
    forget_hbm,
    new_cell,
    new_norm,
    new_stab,
    numer,
    small,
    norm,
    stab,
    queries,
    keys,
    values,
    in_gate,
    forget,
    tiles,
    lhs,
    rhs,
    keep_at,
    small_sems,
    in_sems,
    out_sems,
):
    head, part = pl.program_id(0), pl.program_id(1)
    heads, blocks, seqs = stab.shape
    count, per, rows_k, cols_v = tiles.shape
    parts = count // heads
    rblk = rows_k // blocks

    def fetch(at):
        source = cell.at[pl.ds((at % parts) * per, per), at // parts]
        return pltpu.make_async_copy(source, tiles.at[at], in_sems.at[at])

    def flush(at, group):
        source = tiles.at[at, pl.ds(group * GROUP, GROUP)]
        target = new_cell.at[pl.ds((at % parts) * per + group * GROUP, GROUP), at // parts]
        return pltpu.make_async_copy(source, target, out_sems.at[at, group])

    @pl.when((head == 0) & (part == 0))
    def _():
        pairs = (
            (stab_hbm, stab),
            (in_gate_hbm, in_gate),
            (forget_hbm, forget),
            (norm_hbm, norm),
            (queries_hbm, queries),
            (keys_hbm, keys),
            (values_hbm, values),
        )
        copies = [
            pltpu.make_async_copy(source, target, small_sems.at[index])
            for index, (source, target) in enumerate(pairs)
        ]
        for copy in copies:
            copy.start()
        for ahead in range(AHEAD):
            fetch(ahead).start()
        for copy in copies:
            copy.wait()

    @pl.when(part == 0)
    def _():
        pick = pl.ds(head, seqs, stride=heads)
        gate = in_gate[pl.ds(head, 1), :]
        carried = jax.nn.log_sigmoid(forget[pl.ds(head, 1), :]) + stab[head]
        fresh = jnp.maximum(carried, gate)
        top = jnp.max(fresh, axis=0, keepdims=True)
        new_stab[head] = fresh
        keep8 = jnp.exp(carried - fresh)
        keep_at[...] = keep8

        def spread(small8):
            rows = [jnp.broadcast_to(small8[b : b + 1, :], (rblk, seqs)) for b in range(blocks)]
            return jnp.concatenate(rows, axis=0).T

        write = spread(jnp.exp(gate - fresh)) * (keys[pick, :] * scale)
        weight = spread(jnp.exp(fresh - top)) * queries[pick, :]
        normal = spread(keep8) * norm[pick, :] + write
        new_norm[pick, :] = normal
        small[0, pl.ds(head, 1), :] = top
        small[1, pl.ds(head, 1), :] = jnp.sum((normal * weight).T, axis=0, keepdims=True)
        write_hi, write_lo = two_terms(write)
        weight_hi, weight_lo = two_terms(weight)
        value_hi, value_lo = two_terms(values[pick, :])
        zeros = jnp.zeros((GROUP, cols_v), F32)
        ones = jnp.ones((GROUP, cols_v), F32)
        for group in range(seqs // GROUP):
            rows = slice(group * GROUP, (group + 1) * GROUP)
            left = [write_hi[rows], write_hi[rows], write_lo[rows], weight_hi[rows], weight_lo[rows]]
            outer = [value_hi[rows], value_lo[rows], value_hi[rows], zeros, zeros]
            plain = [zeros, zeros, zeros, ones, ones]
            spare = rows_k // GROUP - len(left)
            stacked = jnp.concatenate(left + [zeros] * spare, axis=0)
            lhs[group] = stacked.T.astype(BF16)
            right = jnp.concatenate(
                [
                    jnp.concatenate(outer + [zeros] * spare, axis=0),
                    jnp.concatenate(plain + [zeros] * spare, axis=0),
                ],
                axis=1,
            )
            rhs[group] = right.astype(BF16)

    at = head * parts + part
    groups = per // GROUP
    keeps = keep_at[:, 0:per]
    for other in range(1, parts):
        keeps = jnp.where(part == other, keep_at[:, other * per : (other + 1) * per], keeps)
    lane = lax.broadcasted_iota(jnp.int32, (rows_k, rows_k), 1) % GROUP

    @pl.when(at + AHEAD < count)
    def _():
        fetch(at + AHEAD).start()

    fetch(at).wait()
    for group in range(groups):
        left, right = lhs[part * groups + group], rhs[part * groups + group]
        for slot in range(GROUP):
            pair = group * GROUP + slot
            mine = jnp.where(lane == slot, left, jnp.zeros_like(left))
            spread = jnp.dot(mine, right, preferred_element_type=F32)
            kept = jnp.broadcast_to(keeps[:, pair : pair + 1], (blocks, cols_v))
            kept = jnp.concatenate(
                [jnp.broadcast_to(kept[b : b + 1, :], (rblk, cols_v)) for b in range(blocks)], axis=0
            )
            fresh_cell = kept * tiles[at, pair] + spread[:, :cols_v]
            tiles[at, pair] = fresh_cell
            numer[pl.ds((part * per + pair) * heads + head, 1), :] = jnp.sum(
                fresh_cell * spread[:, cols_v:], axis=0, keepdims=True
            )
        flush(at, group).start()

    @pl.when(at == count - 1)
    def _():
        for done in range(count):
            for group in range(groups):
                flush(done, group).wait()


def stream(cell, norm, stab, queries, keys, values, in_gate, forget):
    seqs, heads, rows_k, cols_v = cell.shape
    blocks = stab.shape[1]
    parts = seqs // PAIRS
    scale = (rows_k * lax.axis_size("row")) ** (-0.5)

    def whole(array):
        return pl.BlockSpec(array.shape, lambda h, p, n=len(array.shape): (0,) * n)

    out_shape = [
        jax.ShapeDtypeStruct(cell.shape, F32),
        jax.ShapeDtypeStruct(norm.shape, F32),
        jax.ShapeDtypeStruct(stab.shape, F32),
        jax.ShapeDtypeStruct((seqs * heads, cols_v), F32),
        jax.ShapeDtypeStruct((2, heads, seqs), F32),
    ]
    rest = (norm, stab, queries, keys, values, in_gate, forget)
    args = [pltpu.with_memory_space_constraint(a, pltpu.HBM) for a in (cell, *rest)]
    return pl.pallas_call(
        functools.partial(stream_kernel, scale),
        grid=(heads, parts),
        in_specs=[HBM_SPEC] * len(args),
        out_specs=[HBM_SPEC] + [whole(a) for a in out_shape[1:]],
        out_shape=out_shape,
        scratch_shapes=[pltpu.VMEM(a.shape, F32) for a in rest]
        + [
            pltpu.VMEM((heads * parts, PAIRS, rows_k, cols_v), F32),
            pltpu.VMEM((seqs // GROUP, rows_k, rows_k), BF16),
            pltpu.VMEM((seqs // GROUP, rows_k, 2 * cols_v), BF16),
            pltpu.VMEM((blocks, seqs), F32),
            pltpu.SemaphoreType.DMA((len(rest),)),
            pltpu.SemaphoreType.DMA((heads * parts,)),
            pltpu.SemaphoreType.DMA((heads * parts, PAIRS // GROUP)),
        ],
        compiler_params=pltpu.CompilerParams(
            dimension_semantics=("arbitrary", "arbitrary"), vmem_limit_bytes=44 << 20
        ),
        cost_estimate=pl.CostEstimate(
            flops=200 * cell.size, bytes_accessed=8 * cell.size, transcendentals=0
        ),
    )(*args)


def chunks_of(seqs):
    sizes = [seqs * share // sum(SPLIT) for share in SPLIT]
    return sizes, [sum(sizes[:part]) for part in range(CHUNKS)]


def tail_kernel(
    numer,
    small,
    logits,
    gain,
    weight,
    weight_far,
    layer_out,
    readout,
    numer_in,
    small_in,
    held,
    gate,
    gated,
    stats,
    stats_in,
    parts_out,
    parts_in,
    own,
    mine,
    mine_in,
    small_sems,
    row_sems,
    held_sems,
    stats_sems,
    parts_sems,
    mine_sems,
):
    row, hb, col = lax.axis_index("row"), lax.axis_index("hb"), lax.axis_index("col")
    cols, hbs = lax.axis_size("col"), lax.axis_size("hb")
    heads = small.shape[1]
    count, cols_v = numer.shape
    seqs = count // heads
    width = cols_v * cols
    sizes, firsts = chunks_of(seqs)
    depth, out_cols = weight.shape
    chunk = out_cols // cols
    across = 1 - row
    twin = hb + 1 - 2 * (hb % 2)
    peers = [(col + shift) % cols for shift in range(cols)]

    barrier = pltpu.get_barrier_semaphore()
    pl.semaphore_signal(barrier, inc=1, device_id={"row": across}, device_id_type=MESH)
    pl.semaphore_signal(barrier, inc=1, device_id={"hb": twin}, device_id_type=MESH)
    for shift in range(1, cols):
        pl.semaphore_signal(barrier, inc=1, device_id={"col": peers[shift]}, device_id_type=MESH)

    for seq in range(seqs):
        rows = pl.ds(seq * heads, heads)
        gate[rows, :] = jax.nn.sigmoid(logits[rows, :]) * gain[...]

    pl.semaphore_wait(barrier, 1 + cols)

    def remote(source, target, sems, index, device):
        return pltpu.make_async_remote_copy(
            src_ref=source,
            dst_ref=target,
            send_sem=sems.at[(0,) + index],
            recv_sem=sems.at[(1,) + index],
            device_id=device,
            device_id_type=MESH,
        )

    small_copy = remote(small, small_in, small_sems, (0,), {"row": across})
    small_copy.start()
    row_copies = []
    for part in range(CHUNKS):
        rows = pl.ds(firsts[part] * heads, sizes[part] * heads)
        row_copies.append(
            remote(numer.at[rows, :], numer_in.at[rows, :], row_sems, (part,), {"row": across})
        )
        row_copies[part].start()
    twins = [
        remote(source, held.at[slot], held_sems, (slot,), {"hb": twin})
        for slot, source in enumerate((weight, weight_far))
    ]
    for copy in twins:
        copy.start()

    small_copy.wait()
    joined = jnp.maximum(small[0], small_in[0])
    own_scale = jnp.exp(small[0] - joined)
    other_scale = jnp.exp(small_in[0] - joined)
    denom = small[1] * own_scale + small_in[1] * other_scale
    bound = jnp.maximum(jnp.abs(denom), jnp.exp(-joined))
    own_scale = own_scale / bound
    other_scale = other_scale / bound
    lane = lax.broadcasted_iota(jnp.int32, (heads, cols_v), 1)

    blocks = (weight, weight_far, held.at[0], held.at[1])
    stats_copies, parts_copies, mine_copies = {}, {}, {}

    def combine(part):
        row_copies[part].wait()
        sums = jnp.zeros((heads, cols_v), F32)
        squares = sums
        for seq in range(sizes[part]):
            at = firsts[part] + seq
            rows = pl.ds(at * heads, heads)
            value = (
                numer[rows, :] * own_scale[:, at : at + 1]
                + numer_in[rows, :] * other_scale[:, at : at + 1]
            )
            readout[rows, :] = value
            sums = jnp.where(lane == seq, jnp.sum(value, axis=1, keepdims=True), sums)
            squares = jnp.where(lane == seq, jnp.sum(value * value, axis=1, keepdims=True), squares)
        stats[part, 0] = sums
        stats[part, 1] = squares
        for shift in range(1, cols):
            copy = remote(
                stats.at[part],
                stats_in.at[part, shift - 1],
                stats_sems,
                (part, shift - 1),
                {"col": peers[shift]},
            )
            copy.start()
            stats_copies[part, shift] = copy

    def project(part):
        for shift in range(1, cols):
            stats_copies[part, shift].wait()
        total = functools.reduce(
            lambda a, b: a + b, [stats_in[part, shift] for shift in range(cols - 1)], stats[part]
        )
        mean = total[0] / width
        rate = lax.rsqrt(total[1] / width - mean * mean + 1e-06)
        for seq in range(sizes[part]):
            rows = pl.ds((firsts[part] + seq) * heads, heads)
            gated[rows, :] = (
                (readout[rows, :] - mean[:, seq : seq + 1]) * rate[:, seq : seq + 1] * gate[rows, :]
            )
        if part == 0:
            for copy in twins:
                copy.wait()
        owners = [hb, (hb + 2) % hbs, twin, (twin + 2) % hbs]
        lefts = []
        for owner in owners:
            pieces = [
                gated[
                    pl.ds(
                        firsts[part] * heads + owner * (depth // cols_v) + at,
                        sizes[part],
                        stride=heads,
                    ),
                    :,
                ]
                for at in range(depth // cols_v)
            ]
            lefts.append(jnp.concatenate(pieces, axis=1).astype(BF16))
        for shift in list(range(1, cols)) + [0]:
            start = pl.multiple_of(peers[shift] * chunk, chunk)
            term = None
            for slot, left in enumerate(lefts):
                block = blocks[slot][:, pl.ds(start, chunk)]
                product = jnp.dot(left, block, preferred_element_type=F32)
                term = product if term is None else term + product
            if shift == 0:
                own[pl.ds(firsts[part], sizes[part]), :] = term
                continue
            rows = pl.ds(firsts[part], sizes[part])
            parts_out[shift - 1, rows, :] = term.astype(BF16)
            copy = remote(
                parts_out.at[shift - 1, rows, :],
                parts_in.at[shift - 1, rows, :],
                parts_sems,
                (part, shift - 1),
                {"col": peers[shift]},
            )
            copy.start()
            parts_copies[part, shift] = copy

    def gather(part):
        rows = pl.ds(firsts[part], sizes[part])
        total = own[rows, :]
        for shift in range(1, cols):
            parts_copies[part, shift].wait()
            total = total + parts_in[shift - 1, rows, :].astype(F32)
        total = total.astype(BF16)
        mine[rows, :] = total
        for shift in range(1, cols):
            copy = remote(
                mine.at[rows, :],
                mine_in.at[shift - 1, rows, :],
                mine_sems,
                (part, shift - 1),
                {"col": peers[shift]},
            )
            copy.start()
            mine_copies[part, shift] = copy
        start = pl.multiple_of(col * chunk, chunk)
        layer_out[rows, pl.ds(start, chunk)] = total.astype(F32)

    def finish(part):
        for shift in range(1, cols):
            mine_copies[part, shift].wait()
            start = pl.multiple_of(((col + cols - shift) % cols) * chunk, chunk)
            rows = pl.ds(firsts[part], sizes[part])
            layer_out[rows, pl.ds(start, chunk)] = mine_in[shift - 1, rows, :].astype(F32)

    steps = ((combine, 0), (project, 1), (gather, 2), (finish, 3))
    for tick in range(CHUNKS + 3):
        for step, delay in steps:
            if 0 <= tick - delay < CHUNKS:
                step(tick - delay)


def tail(numer, small, logits, gain, weight, weight_far):
    cols = lax.axis_size("col")
    count, cols_v = numer.shape
    heads, seqs = small.shape[1:]
    depth, out_cols = weight.shape
    chunk = out_cols // cols
    sems = lambda *shape: pltpu.SemaphoreType.DMA((2,) + shape)
    return pl.pallas_call(
        tail_kernel,
        in_specs=[VMEM_SPEC] * 6,
        out_specs=[VMEM_SPEC] * 2,
        out_shape=[
            jax.ShapeDtypeStruct((seqs, out_cols), F32),
            jax.ShapeDtypeStruct((count, cols_v), F32),
        ],
        scratch_shapes=[
            pltpu.VMEM((count, cols_v), F32),
            pltpu.VMEM(small.shape, F32),
            pltpu.VMEM((2, depth, out_cols), BF16),
            pltpu.VMEM((count, cols_v), F32),
            pltpu.VMEM((count, cols_v), F32),
            pltpu.VMEM((CHUNKS, 2, heads, cols_v), F32),
            pltpu.VMEM((CHUNKS, cols - 1, 2, heads, cols_v), F32),
            pltpu.VMEM((cols - 1, seqs, chunk), BF16),
            pltpu.VMEM((cols - 1, seqs, chunk), BF16),
            pltpu.VMEM((seqs, chunk), F32),
            pltpu.VMEM((seqs, chunk), BF16),
            pltpu.VMEM((cols - 1, seqs, chunk), BF16),
            sems(1),
            sems(CHUNKS),
            sems(2),
            sems(CHUNKS, cols - 1),
            sems(CHUNKS, cols - 1),
            sems(CHUNKS, cols - 1),
        ],
        compiler_params=pltpu.CompilerParams(
            vmem_limit_bytes=24 << 20, collective_id=0, has_side_effects=True
        ),
        cost_estimate=pl.CostEstimate(
            flops=2 * seqs * 4 * depth * out_cols,
            bytes_accessed=8 * depth * out_cols,
            transcendentals=0,
        ),
    )(numer, small, logits, gain, weight, weight_far)


def settle_kernel(layer_out, readout, layer_hbm, readout_hbm, sems):
    copies = [
        pltpu.make_async_copy(source, target, sems.at[index])
        for index, (source, target) in enumerate(((layer_out, layer_hbm), (readout, readout_hbm)))
    ]
    for copy in copies:
        copy.start()
    for copy in copies:
        copy.wait()


def settle(layer_out, readout):
    return pl.pallas_call(
        settle_kernel,
        in_specs=[VMEM_SPEC] * 2,
        out_specs=[pl.BlockSpec(memory_space=pl.ANY)] * 2,
        out_shape=[jax.ShapeDtypeStruct(a.shape, F32) for a in (layer_out, readout)],
        scratch_shapes=[pltpu.SemaphoreType.DMA((2,))],
        compiler_params=pltpu.CompilerParams(vmem_limit_bytes=4 << 20),
    )(layer_out, readout)


def fused(
    cell_state,
    normalizer,
    stabilizer,
    queries,
    key_vectors,
    token_value_vectors,
    input_gate,
    forget_gate,
    output_gate_logits,
    norm_gain,
    out_weight,
):
    seqs, heads, rows_k, cols_v = cell_state.shape
    flat = lambda a: a.reshape((seqs * heads,) + a.shape[2:])
    weight = out_weight.reshape(-1, out_weight.shape[2])
    weight_far = lax.ppermute(weight, "hb", [(i, (i + 2) % 4) for i in range(4)])
    refreshed_cell, new_normal, fresh, numer, small = stream(
        cell_state,
        flat(normalizer),
        stabilizer.transpose(1, 2, 0),
        flat(queries),
        flat(key_vectors),
        flat(token_value_vectors),
        input_gate.T,
        forget_gate.T,
    )
    layer_out, readout = settle(
        *tail(numer, small, flat(output_gate_logits), norm_gain, weight, weight_far)
    )
    return (
        layer_out,
        readout.reshape(seqs, heads, cols_v),
        refreshed_cell,
        new_normal.reshape(normalizer.shape),
        fresh.transpose(2, 0, 1),
    )


def fits(cell_state, out_weight):
    seqs, heads, rows_k, cols_v = cell_state.shape
    sizes = tuple(lax.axis_size(axis) for axis in ("hb", "row", "col"))
    return (
        sizes == (4, 2, 4)
        and heads == 8
        and rows_k == cols_v == 128
        and seqs % max(PAIRS, sum(SPLIT) * GROUP) == 0
        and seqs <= 128
        and out_weight.shape[0] * sizes[0] == heads
        and out_weight.shape[2] % (128 * sizes[2]) == 0
    )


def local(
    cell_state,
    normalizer,
    stabilizer,
    queries,
    key_vectors,
    token_value_vectors,
    input_gate,
    forget_gate,
    output_gate_logits,
    norm_gain,
    out_weight,
):
    if fits(cell_state, out_weight):
        return fused(
            cell_state,
            normalizer,
            stabilizer,
            queries,
            key_vectors,
            token_value_vectors,
            input_gate,
            forget_gate,
            output_gate_logits,
            norm_gain,
            out_weight,
        )
    seqs, heads, rows_k, cols_v = cell_state.shape
    rblk = rows_k // stabilizer.shape[2]
    scale = (rows_k * lax.axis_size("row")) ** (-0.5)
    carried = jax.nn.log_sigmoid(forget_gate)[:, :, None] + stabilizer
    fresh = jnp.maximum(carried, input_gate[:, :, None])
    keep8 = jnp.exp(carried - fresh)
    admit8 = jnp.exp(input_gate[:, :, None] - fresh)
    local_top = jnp.max(fresh, axis=2)
    keep = jnp.repeat(keep8, rblk, axis=2)
    write = jnp.repeat(admit8, rblk, axis=2) * key_vectors * scale
    refreshed_cell = (
        keep[:, :, :, None] * cell_state
        + write[:, :, :, None] * token_value_vectors[:, :, None, :]
    )
    new_normal = keep * normalizer + write
    weight = jnp.repeat(jnp.exp(fresh - local_top[:, :, None]), rblk, axis=2) * queries
    numerator = jnp.einsum(
        "bhkv,bhk->bhv", refreshed_cell, weight, precision=lax.Precision.HIGHEST
    )
    denom = jnp.sum(new_normal * weight, axis=2)
    top, numerator, denom = combined_all((local_top, numerator, denom), "row", combine_pairs)
    readout = numerator / jnp.maximum(jnp.abs(denom), jnp.exp(-top))[:, :, None]
    stats = jnp.stack([jnp.sum(readout, axis=2), jnp.sum(readout * readout, axis=2)])
    cols = lax.axis_size("col")
    sums = lax.psum(stats, "col")
    mean = sums[0] / (cols_v * cols)
    var = sums[1] / (cols_v * cols) - mean * mean
    normed = (readout - mean[:, :, None]) * lax.rsqrt(var + 1e-06)[:, :, None]
    gated = (normed * norm_gain * jax.nn.sigmoid(output_gate_logits)).astype(BF16)
    gated = gated.reshape(seqs, -1)
    out_cols = out_weight.shape[2]
    partial_value = jnp.dot(
        gated,
        lax.all_gather(out_weight, "hb", axis=0, tiled=True).reshape(-1, out_cols),
        preferred_element_type=F32,
    )
    layer_out = lax.psum(partial_value, "col")
    return (layer_out, readout, refreshed_cell, new_normal, fresh)


def solution(mesh):
    placed = (
        P("hb", None, "row", "col"),
        P("hb", None, "row"),
        P("hb", None, "row"),
        P("hb", None, "row"),
        P("hb", None, "row"),
        P("hb", None, "col"),
        P("hb", None),
        P("hb", None),
        P("hb", None, "col"),
        P(None, "col"),
        P("hb", "col", "row"),
    )
    return jax.shard_map(
        local,
        mesh=mesh,
        in_specs=placed,
        out_specs=(
            P("hb", "row"),
            P("hb", None, "col"),
            P("hb", None, "row", "col"),
            P("hb", None, "row"),
            P("hb", None, "row"),
        ),
        check_vma=False,
    )
```

```python
import functools

import jax
import jax.numpy as jnp
from jax import lax
from jax.experimental import pallas as pl
from jax.experimental.pallas import tpu as pltpu
from jax.sharding import PartitionSpec as P

PAIRS = 64
F32 = jnp.float32
BF16 = jnp.bfloat16


def combined_all(part, axis, combine):
    gathered = jax.tree.map(lambda a: lax.all_gather(a, axis), part)

    def take(source):
        return jax.tree.map(lambda a: lax.dynamic_index_in_dim(a, source, 0, False), gathered)

    return lax.fori_loop(
        1, lax.axis_size(axis), lambda source, state: combine(state, take(source)), take(0)
    )


def combine_pairs(left_pair, right_pair):
    joined = jnp.maximum(left_pair[0], right_pair[0])
    left_scale = jnp.exp(left_pair[0] - joined)
    right_scale = jnp.exp(right_pair[0] - joined)
    numerator = left_pair[1] * left_scale[:, :, None] + right_pair[1] * right_scale[:, :, None]
    denom = left_pair[2] * left_scale + right_pair[2] * right_scale
    return (joined, numerator, denom)


MESH = pl.DeviceIdType.MESH
SPLIT = (2, 2)
CHUNKS = len(SPLIT)
GROUP = 16
AHEAD = 3
VMEM_SPEC = pl.BlockSpec(memory_space=pltpu.VMEM)
HBM_SPEC = pl.BlockSpec(memory_space=pltpu.HBM)


def two_terms(array):
    high = array.astype(BF16).astype(F32)
    return high, (array - high).astype(BF16).astype(F32)


def stream_kernel(
    scale,
    cell,
    norm_hbm,
    stab_hbm,
    queries_hbm,
    keys_hbm,
    values_hbm,
    in_gate_hbm,
    forget_hbm,
    new_cell,
    new_norm,
    new_stab,
    numer,
    small,
    norm,
    stab,
    queries,
    keys,
    values,
    in_gate,
    forget,
    tiles,
    lhs,
    rhs,
    keep_at,
    small_sems,
    in_sems,
    out_sems,
):
    head, part = pl.program_id(0), pl.program_id(1)
    heads, blocks, seqs = stab.shape
    count, per, rows_k, cols_v = tiles.shape
    parts = count // heads
    rblk = rows_k // blocks

    def fetch(at):
        source = cell.at[pl.ds((at % parts) * per, per), at // parts]
        return pltpu.make_async_copy(source, tiles.at[at], in_sems.at[at])

    def flush(at, group):
        source = tiles.at[at, pl.ds(group * GROUP, GROUP)]
        target = new_cell.at[pl.ds((at % parts) * per + group * GROUP, GROUP), at // parts]
        return pltpu.make_async_copy(source, target, out_sems.at[at, group])

    @pl.when((head == 0) & (part == 0))
    def _():
        pairs = (
            (stab_hbm, stab),
            (in_gate_hbm, in_gate),
            (forget_hbm, forget),
            (norm_hbm, norm),
            (queries_hbm, queries),
            (keys_hbm, keys),
            (values_hbm, values),
        )
        copies = [
            pltpu.make_async_copy(source, target, small_sems.at[index])
            for index, (source, target) in enumerate(pairs)
        ]
        for copy in copies:
            copy.start()
        for ahead in range(AHEAD):
            fetch(ahead).start()
        for copy in copies:
            copy.wait()

    @pl.when(part == 0)
    def _():
        pick = pl.ds(head, seqs, stride=heads)
        gate = in_gate[pl.ds(head, 1), :]
        carried = jax.nn.log_sigmoid(forget[pl.ds(head, 1), :]) + stab[head]
        fresh = jnp.maximum(carried, gate)
        top = jnp.max(fresh, axis=0, keepdims=True)
        new_stab[head] = fresh
        keep8 = jnp.exp(carried - fresh)
        keep_at[...] = keep8

        def spread(small8):
            rows = [jnp.broadcast_to(small8[b : b + 1, :], (rblk, seqs)) for b in range(blocks)]
            return jnp.concatenate(rows, axis=0).T

        write = spread(jnp.exp(gate - fresh)) * (keys[pick, :] * scale)
        weight = spread(jnp.exp(fresh - top)) * queries[pick, :]
        normal = spread(keep8) * norm[pick, :] + write
        new_norm[pick, :] = normal
        small[0, pl.ds(head, 1), :] = top
        small[1, pl.ds(head, 1), :] = jnp.sum((normal * weight).T, axis=0, keepdims=True)
        write_hi, write_lo = two_terms(write)
        weight_hi, weight_lo = two_terms(weight)
        value_hi, value_lo = two_terms(values[pick, :])
        zeros = jnp.zeros((GROUP, cols_v), F32)
        ones = jnp.ones((GROUP, cols_v), F32)
        for group in range(seqs // GROUP):
            rows = slice(group * GROUP, (group + 1) * GROUP)
            left = [write_hi[rows], write_hi[rows], write_lo[rows], weight_hi[rows], weight_lo[rows]]
            outer = [value_hi[rows], value_lo[rows], value_hi[rows], zeros, zeros]
            plain = [zeros, zeros, zeros, ones, ones]
            spare = rows_k // GROUP - len(left)
            stacked = jnp.concatenate(left + [zeros] * spare, axis=0)
            lhs[group] = stacked.T.astype(BF16)
            right = jnp.concatenate(
                [
                    jnp.concatenate(outer + [zeros] * spare, axis=0),
                    jnp.concatenate(plain + [zeros] * spare, axis=0),
                ],
                axis=1,
            )
            rhs[group] = right.astype(BF16)

    at = head * parts + part
    groups = per // GROUP
    keeps = keep_at[:, 0:per]
    for other in range(1, parts):
        keeps = jnp.where(part == other, keep_at[:, other * per : (other + 1) * per], keeps)
    lane = lax.broadcasted_iota(jnp.int32, (rows_k, rows_k), 1) % GROUP

    @pl.when(at + AHEAD < count)
    def _():
        fetch(at + AHEAD).start()

    fetch(at).wait()
    for group in range(groups):
        left, right = lhs[part * groups + group], rhs[part * groups + group]
        for slot in range(GROUP):
            pair = group * GROUP + slot
            mine = jnp.where(lane == slot, left, jnp.zeros_like(left))
            spread = jnp.dot(mine, right, preferred_element_type=F32)
            kept = jnp.broadcast_to(keeps[:, pair : pair + 1], (blocks, cols_v))
            kept = jnp.concatenate(
                [jnp.broadcast_to(kept[b : b + 1, :], (rblk, cols_v)) for b in range(blocks)], axis=0
            )
            fresh_cell = kept * tiles[at, pair] + spread[:, :cols_v]
            tiles[at, pair] = fresh_cell
            numer[pl.ds((part * per + pair) * heads + head, 1), :] = jnp.sum(
                fresh_cell * spread[:, cols_v:], axis=0, keepdims=True
            )
        flush(at, group).start()

    @pl.when(at == count - 1)
    def _():
        for done in range(count):
            for group in range(groups):
                flush(done, group).wait()


def stream(cell, norm, stab, queries, keys, values, in_gate, forget):
    seqs, heads, rows_k, cols_v = cell.shape
    blocks = stab.shape[1]
    parts = seqs // PAIRS
    scale = (rows_k * lax.axis_size("row")) ** (-0.5)

    def whole(array):
        return pl.BlockSpec(array.shape, lambda h, p, n=len(array.shape): (0,) * n)

    out_shape = [
        jax.ShapeDtypeStruct(cell.shape, F32),
        jax.ShapeDtypeStruct(norm.shape, F32),
        jax.ShapeDtypeStruct(stab.shape, F32),
        jax.ShapeDtypeStruct((seqs * heads, cols_v), F32),
        jax.ShapeDtypeStruct((2, heads, seqs), F32),
    ]
    rest = (norm, stab, queries, keys, values, in_gate, forget)
    args = [pltpu.with_memory_space_constraint(a, pltpu.HBM) for a in (cell, *rest)]
    return pl.pallas_call(
        functools.partial(stream_kernel, scale),
        grid=(heads, parts),
        in_specs=[HBM_SPEC] * len(args),
        out_specs=[HBM_SPEC] + [whole(a) for a in out_shape[1:]],
        out_shape=out_shape,
        scratch_shapes=[pltpu.VMEM(a.shape, F32) for a in rest]
        + [
            pltpu.VMEM((heads * parts, PAIRS, rows_k, cols_v), F32),
            pltpu.VMEM((seqs // GROUP, rows_k, rows_k), BF16),
            pltpu.VMEM((seqs // GROUP, rows_k, 2 * cols_v), BF16),
            pltpu.VMEM((blocks, seqs), F32),
            pltpu.SemaphoreType.DMA((len(rest),)),
            pltpu.SemaphoreType.DMA((heads * parts,)),
            pltpu.SemaphoreType.DMA((heads * parts, PAIRS // GROUP)),
        ],
        compiler_params=pltpu.CompilerParams(
            dimension_semantics=("arbitrary", "arbitrary"), vmem_limit_bytes=44 << 20
        ),
        cost_estimate=pl.CostEstimate(
            flops=200 * cell.size, bytes_accessed=8 * cell.size, transcendentals=0
        ),
    )(*args)


def chunks_of(seqs):
    sizes = [seqs * share // sum(SPLIT) for share in SPLIT]
    return sizes, [sum(sizes[:part]) for part in range(CHUNKS)]


def tail_kernel(
    numer,
    small,
    logits,
    gain,
    weight,
    weight_far,
    layer_out,
    readout,
    numer_in,
    small_in,
    held,
    gate,
    gated,
    stats,
    stats_in,
    parts_out,
    parts_in,
    own,
    mine,
    mine_in,
    small_sems,
    row_sems,
    held_sems,
    stats_sems,
    parts_sems,
    mine_sems,
):
    row, hb, col = lax.axis_index("row"), lax.axis_index("hb"), lax.axis_index("col")
    cols, hbs = lax.axis_size("col"), lax.axis_size("hb")
    heads = small.shape[1]
    count, cols_v = numer.shape
    seqs = count // heads
    width = cols_v * cols
    sizes, firsts = chunks_of(seqs)
    depth, out_cols = weight.shape
    chunk = out_cols // cols
    across = 1 - row
    twin = hb + 1 - 2 * (hb % 2)
    peers = [(col + shift) % cols for shift in range(cols)]

    barrier = pltpu.get_barrier_semaphore()
    pl.semaphore_signal(barrier, inc=1, device_id={"row": across}, device_id_type=MESH)
    pl.semaphore_signal(barrier, inc=1, device_id={"hb": twin}, device_id_type=MESH)
    for shift in range(1, cols):
        pl.semaphore_signal(barrier, inc=1, device_id={"col": peers[shift]}, device_id_type=MESH)


    pl.semaphore_wait(barrier, 1 + cols)

    def remote(source, target, sems, index, device):
        return pltpu.make_async_remote_copy(
            src_ref=source,
            dst_ref=target,
            send_sem=sems.at[(0,) + index],
            recv_sem=sems.at[(1,) + index],
            device_id=device,
            device_id_type=MESH,
        )

    small_copy = remote(small, small_in, small_sems, (0,), {"row": across})
    small_copy.start()
    row_copies = []
    for part in range(CHUNKS):
        rows = pl.ds(firsts[part] * heads, sizes[part] * heads)
        row_copies.append(
            remote(numer.at[rows, :], numer_in.at[rows, :], row_sems, (part,), {"row": across})
        )
        row_copies[part].start()
    twins = [
        remote(source, held.at[slot], held_sems, (slot,), {"hb": twin})
        for slot, source in enumerate((weight, weight_far))
    ]
    for copy in twins:
        copy.start()

    for seq in range(seqs):
        rows = pl.ds(seq * heads, heads)
        gate[rows, :] = jax.nn.sigmoid(logits[rows, :]) * gain[...]

    small_copy.wait()
    joined = jnp.maximum(small[0], small_in[0])
    own_scale = jnp.exp(small[0] - joined)
    other_scale = jnp.exp(small_in[0] - joined)
    denom = small[1] * own_scale + small_in[1] * other_scale
    bound = jnp.maximum(jnp.abs(denom), jnp.exp(-joined))
    own_scale = own_scale / bound
    other_scale = other_scale / bound
    lane = lax.broadcasted_iota(jnp.int32, (heads, cols_v), 1)

    blocks = (weight, weight_far, held.at[0], held.at[1])
    stats_copies, parts_copies, mine_copies = {}, {}, {}

    def combine(part):
        row_copies[part].wait()
        sums = jnp.zeros((heads, cols_v), F32)
        squares = sums
        for seq in range(sizes[part]):
            at = firsts[part] + seq
            rows = pl.ds(at * heads, heads)
            value = (
                numer[rows, :] * own_scale[:, at : at + 1]
                + numer_in[rows, :] * other_scale[:, at : at + 1]
            )
            readout[rows, :] = value
            sums = jnp.where(lane == seq, jnp.sum(value, axis=1, keepdims=True), sums)
            squares = jnp.where(lane == seq, jnp.sum(value * value, axis=1, keepdims=True), squares)
        stats[part, 0] = sums
        stats[part, 1] = squares
        for shift in range(1, cols):
            copy = remote(
                stats.at[part],
                stats_in.at[part, shift - 1],
                stats_sems,
                (part, shift - 1),
                {"col": peers[shift]},
            )
            copy.start()
            stats_copies[part, shift] = copy

    def project(part):
        for shift in range(1, cols):
            stats_copies[part, shift].wait()
        total = functools.reduce(
            lambda a, b: a + b, [stats_in[part, shift] for shift in range(cols - 1)], stats[part]
        )
        mean = total[0] / width
        rate = lax.rsqrt(total[1] / width - mean * mean + 1e-06)
        for seq in range(sizes[part]):
            rows = pl.ds((firsts[part] + seq) * heads, heads)
            gated[rows, :] = (
                (readout[rows, :] - mean[:, seq : seq + 1]) * rate[:, seq : seq + 1] * gate[rows, :]
            )
        if part == 0:
            for copy in twins:
                copy.wait()
        owners = [hb, (hb + 2) % hbs, twin, (twin + 2) % hbs]
        lefts = []
        for owner in owners:
            pieces = [
                gated[
                    pl.ds(
                        firsts[part] * heads + owner * (depth // cols_v) + at,
                        sizes[part],
                        stride=heads,
                    ),
                    :,
                ]
                for at in range(depth // cols_v)
            ]
            lefts.append(jnp.concatenate(pieces, axis=1).astype(BF16))
        for shift in list(range(1, cols)) + [0]:
            start = pl.multiple_of(peers[shift] * chunk, chunk)
            term = None
            for slot, left in enumerate(lefts):
                block = blocks[slot][:, pl.ds(start, chunk)]
                product = jnp.dot(left, block, preferred_element_type=F32)
                term = product if term is None else term + product
            if shift == 0:
                own[pl.ds(firsts[part], sizes[part]), :] = term
                continue
            rows = pl.ds(firsts[part], sizes[part])
            parts_out[shift - 1, rows, :] = term.astype(BF16)
            copy = remote(
                parts_out.at[shift - 1, rows, :],
                parts_in.at[shift - 1, rows, :],
                parts_sems,
                (part, shift - 1),
                {"col": peers[shift]},
            )
            copy.start()
            parts_copies[part, shift] = copy

    def gather(part):
        rows = pl.ds(firsts[part], sizes[part])
        total = own[rows, :]
        for shift in range(1, cols):
            parts_copies[part, shift].wait()
            total = total + parts_in[shift - 1, rows, :].astype(F32)
        total = total.astype(BF16)
        mine[rows, :] = total
        for shift in range(1, cols):
            copy = remote(
                mine.at[rows, :],
                mine_in.at[shift - 1, rows, :],
                mine_sems,
                (part, shift - 1),
                {"col": peers[shift]},
            )
            copy.start()
            mine_copies[part, shift] = copy
        start = pl.multiple_of(col * chunk, chunk)
        layer_out[rows, pl.ds(start, chunk)] = total.astype(F32)

    def finish(part):
        for shift in range(1, cols):
            mine_copies[part, shift].wait()
            start = pl.multiple_of(((col + cols - shift) % cols) * chunk, chunk)
            rows = pl.ds(firsts[part], sizes[part])
            layer_out[rows, pl.ds(start, chunk)] = mine_in[shift - 1, rows, :].astype(F32)

    steps = ((combine, 0), (project, 1), (gather, 2), (finish, 3))
    for tick in range(CHUNKS + 3):
        for step, delay in steps:
            if 0 <= tick - delay < CHUNKS:
                step(tick - delay)


def tail(numer, small, logits, gain, weight, weight_far):
    cols = lax.axis_size("col")
    count, cols_v = numer.shape
    heads, seqs = small.shape[1:]
    depth, out_cols = weight.shape
    chunk = out_cols // cols
    sems = lambda *shape: pltpu.SemaphoreType.DMA((2,) + shape)
    return pl.pallas_call(
        tail_kernel,
        in_specs=[VMEM_SPEC] * 6,
        out_specs=[VMEM_SPEC] * 2,
        out_shape=[
            jax.ShapeDtypeStruct((seqs, out_cols), F32),
            jax.ShapeDtypeStruct((count, cols_v), F32),
        ],
        scratch_shapes=[
            pltpu.VMEM((count, cols_v), F32),
            pltpu.VMEM(small.shape, F32),
            pltpu.VMEM((2, depth, out_cols), BF16),
            pltpu.VMEM((count, cols_v), F32),
            pltpu.VMEM((count, cols_v), F32),
            pltpu.VMEM((CHUNKS, 2, heads, cols_v), F32),
            pltpu.VMEM((CHUNKS, cols - 1, 2, heads, cols_v), F32),
            pltpu.VMEM((cols - 1, seqs, chunk), BF16),
            pltpu.VMEM((cols - 1, seqs, chunk), BF16),
            pltpu.VMEM((seqs, chunk), F32),
            pltpu.VMEM((seqs, chunk), BF16),
            pltpu.VMEM((cols - 1, seqs, chunk), BF16),
            sems(1),
            sems(CHUNKS),
            sems(2),
            sems(CHUNKS, cols - 1),
            sems(CHUNKS, cols - 1),
            sems(CHUNKS, cols - 1),
        ],
        compiler_params=pltpu.CompilerParams(
            vmem_limit_bytes=24 << 20, collective_id=0, has_side_effects=True
        ),
        cost_estimate=pl.CostEstimate(
            flops=2 * seqs * 4 * depth * out_cols,
            bytes_accessed=8 * depth * out_cols,
            transcendentals=0,
        ),
    )(numer, small, logits, gain, weight, weight_far)


def settle_kernel(layer_out, readout, layer_hbm, readout_hbm, sems):
    copies = [
        pltpu.make_async_copy(source, target, sems.at[index])
        for index, (source, target) in enumerate(((layer_out, layer_hbm), (readout, readout_hbm)))
    ]
    for copy in copies:
        copy.start()
    for copy in copies:
        copy.wait()


def settle(layer_out, readout):
    return pl.pallas_call(
        settle_kernel,
        in_specs=[VMEM_SPEC] * 2,
        out_specs=[pl.BlockSpec(memory_space=pl.ANY)] * 2,
        out_shape=[jax.ShapeDtypeStruct(a.shape, F32) for a in (layer_out, readout)],
        scratch_shapes=[pltpu.SemaphoreType.DMA((2,))],
        compiler_params=pltpu.CompilerParams(vmem_limit_bytes=4 << 20),
    )(layer_out, readout)


def fused(
    cell_state,
    normalizer,
    stabilizer,
    queries,
    key_vectors,
    token_value_vectors,
    input_gate,
    forget_gate,
    output_gate_logits,
    norm_gain,
    out_weight,
):
    seqs, heads, rows_k, cols_v = cell_state.shape
    flat = lambda a: a.reshape((seqs * heads,) + a.shape[2:])
    weight = out_weight.reshape(-1, out_weight.shape[2])
    weight_far = lax.ppermute(weight, "hb", [(i, (i + 2) % 4) for i in range(4)])
    refreshed_cell, new_normal, fresh, numer, small = stream(
        cell_state,
        flat(normalizer),
        stabilizer.transpose(1, 2, 0),
        flat(queries),
        flat(key_vectors),
        flat(token_value_vectors),
        input_gate.T,
        forget_gate.T,
    )
    layer_out, readout = settle(
        *tail(numer, small, flat(output_gate_logits), norm_gain, weight, weight_far)
    )
    return (
        layer_out,
        readout.reshape(seqs, heads, cols_v),
        refreshed_cell,
        new_normal.reshape(normalizer.shape),
        fresh.transpose(2, 0, 1),
    )


def fits(cell_state, out_weight):
    seqs, heads, rows_k, cols_v = cell_state.shape
    sizes = tuple(lax.axis_size(axis) for axis in ("hb", "row", "col"))
    return (
        sizes == (4, 2, 4)
        and heads == 8
        and rows_k == cols_v == 128
        and seqs % max(PAIRS, sum(SPLIT) * GROUP) == 0
        and seqs <= 128
        and out_weight.shape[0] * sizes[0] == heads
        and out_weight.shape[2] % (128 * sizes[2]) == 0
    )


def local(
    cell_state,
    normalizer,
    stabilizer,
    queries,
    key_vectors,
    token_value_vectors,
    input_gate,
    forget_gate,
    output_gate_logits,
    norm_gain,
    out_weight,
):
    if fits(cell_state, out_weight):
        return fused(
            cell_state,
            normalizer,
            stabilizer,
            queries,
            key_vectors,
            token_value_vectors,
            input_gate,
            forget_gate,
            output_gate_logits,
            norm_gain,
            out_weight,
        )
    seqs, heads, rows_k, cols_v = cell_state.shape
    rblk = rows_k // stabilizer.shape[2]
    scale = (rows_k * lax.axis_size("row")) ** (-0.5)
    carried = jax.nn.log_sigmoid(forget_gate)[:, :, None] + stabilizer
    fresh = jnp.maximum(carried, input_gate[:, :, None])
    keep8 = jnp.exp(carried - fresh)
    admit8 = jnp.exp(input_gate[:, :, None] - fresh)
    local_top = jnp.max(fresh, axis=2)
    keep = jnp.repeat(keep8, rblk, axis=2)
    write = jnp.repeat(admit8, rblk, axis=2) * key_vectors * scale
    refreshed_cell = (
        keep[:, :, :, None] * cell_state
        + write[:, :, :, None] * token_value_vectors[:, :, None, :]
    )
    new_normal = keep * normalizer + write
    weight = jnp.repeat(jnp.exp(fresh - local_top[:, :, None]), rblk, axis=2) * queries
    numerator = jnp.einsum(
        "bhkv,bhk->bhv", refreshed_cell, weight, precision=lax.Precision.HIGHEST
    )
    denom = jnp.sum(new_normal * weight, axis=2)
    top, numerator, denom = combined_all((local_top, numerator, denom), "row", combine_pairs)
    readout = numerator / jnp.maximum(jnp.abs(denom), jnp.exp(-top))[:, :, None]
    stats = jnp.stack([jnp.sum(readout, axis=2), jnp.sum(readout * readout, axis=2)])
    cols = lax.axis_size("col")
    sums = lax.psum(stats, "col")
    mean = sums[0] / (cols_v * cols)
    var = sums[1] / (cols_v * cols) - mean * mean
    normed = (readout - mean[:, :, None]) * lax.rsqrt(var + 1e-06)[:, :, None]
    gated = (normed * norm_gain * jax.nn.sigmoid(output_gate_logits)).astype(BF16)
    gated = gated.reshape(seqs, -1)
    out_cols = out_weight.shape[2]
    partial_value = jnp.dot(
        gated,
        lax.all_gather(out_weight, "hb", axis=0, tiled=True).reshape(-1, out_cols),
        preferred_element_type=F32,
    )
    layer_out = lax.psum(partial_value, "col")
    return (layer_out, readout, refreshed_cell, new_normal, fresh)


def solution(mesh):
    placed = (
        P("hb", None, "row", "col"),
        P("hb", None, "row"),
        P("hb", None, "row"),
        P("hb", None, "row"),
        P("hb", None, "row"),
        P("hb", None, "col"),
        P("hb", None),
        P("hb", None),
        P("hb", None, "col"),
        P(None, "col"),
        P("hb", "col", "row"),
    )
    return jax.shard_map(
        local,
        mesh=mesh,
        in_specs=placed,
        out_specs=(
            P("hb", "row"),
            P("hb", None, "col"),
            P("hb", None, "row", "col"),
            P("hb", None, "row"),
            P("hb", None, "row"),
        ),
        check_vma=False,
    )
```
